32 devices in a mesh: ep: 16 (over z, x, core), dp: 2 (over y).
Axes of the slice: x: 2, y: 2, z: 4, core: 2. Of those that a mesh axis runs over, the one named last changes fastest.
Arguments:
- tokens: bfloat16 [2048, 1024], P(('dp', 'ep')), parts along dimension 0, may hold values from -6 to 6
- norm_gain: float32 [1024], replicated, may hold values from 0.1 to 1.9
- router_weight: bfloat16 [1024, 16], replicated, may hold values from -0.1875 to 0.1875
- expert_ids: int32 [2048, 2], P(('dp', 'ep')), parts along dimension 0, may hold values from 0 to 15, all different within a row; in each aligned block of 64 rows (0 to 63, 64 to 127, ...) at most 32 rows name the same one
- w_gate: bfloat16 [16, 1024, 512], P('ep'), may hold values from -0.1875 to 0.1875
- w_up: bfloat16 [16, 1024, 512], P('ep'), may hold values from -0.1875 to 0.1875
- w_down: bfloat16 [16, 512, 1024], P('ep'), may hold values from -0.25 to 0.25
Outputs:
- moe_out: bfloat16 [2048, 1024], P(('dp', 'ep')), parts along dimension 0
The draws below stay inside these ranges and needn't reach their ends.
There are 2 independent parts, one for each index of `dp`. The reference program is written for one: setup_inputs(seed, part) draws one part's arguments, and reference() takes and returns one part's arrays. A program takes and returns all parts, laid end to end along the dimension named above; an argument that names none is the same for every part. Nothing has to cross between parts.
Inputs may be any that keep to these rules, and one draw needn't show every extreme that they name: Each row of expert_ids names 2 different experts of 0 to 15; within the rows of one device (aligned blocks of 64 rows) no expert is named more than 32 times, and in some block one expert is named exactly 32 times.
All inputs are finite; a program needn't handle non-finite values.
Results may differ from the reference program's by a relative error of at most 0.0015.
Values may be sent and summed in bfloat16 or wider, within the bound.
A program may use at most 64 MiB of HBM per device.

```python
import math
import jax
import jax.numpy as jnp
import numpy as np
from jax import lax

D = 1024
FF = 512
TOP = 2
TOK_DEV = 64
EXPERTS = 16
TOKENS = 1024
CAP = 32
N_EP = 16


def level_of(stream_key, shape, cuts, low, largest):
    def one(position, parts):
        heights = jax.random.uniform(jax.random.fold_in(jax.random.fold_in(stream_key, 6), position), (parts,), jnp.float32, low / len(cuts), largest / len(cuts))
        return jnp.repeat(jnp.exp(heights), shape[position] // parts).reshape((-1,) + (1,) * (len(shape) - position - 1))

    loudness = one(*cuts[0])
    for cut in cuts[1:]:
        loudness = loudness * one(*cut)
    return loudness


def shared_out(own_key, own, number, rows, number_of, top, limit, lean):
    ranking = jax.random.permutation(own_key, number_of)
    packed, ordinary = load_shares(number_of, rows * top, limit, lean, True), load_shares(number_of, rows * top, limit, lean, False)
    places = jnp.arange(number_of)

    def named(sizes, offset_by):
        used = int((sizes > 0).sum())
        fixed = max(1, used // 4)
        moved = fixed + (places - fixed + offset_by * (used - fixed)) % max(1, number_of - fixed)
        return jnp.zeros((number_of,), jnp.int32).at[ranking[jnp.where(places < fixed, places, moved)]].set(jnp.asarray(sizes, jnp.int32))

    sizes = jnp.where(number % 4 == 0, named(packed, number // 4), named(ordinary, number - number // 4 - 1))
    mixed = jax.random.permutation(jax.random.fold_in(own, 3), number_of)
    donor, taker = mixed[0:number_of // 2 * 2:2], mixed[1:number_of // 2 * 2:2]
    margin = jnp.minimum(sizes[donor] - 1, limit - sizes[taker]) // 2
    margin = jnp.where((donor == ranking[0]) | (taker == ranking[0]) | (sizes[taker] == 0), 0, jnp.maximum(margin, 0))
    moved = jax.random.randint(jax.random.fold_in(own, 4), (number_of // 2,), 0, 1 << 20) % (margin + 1)
    sizes = sizes.at[donor].add(-moved).at[taker].add(moved)
    labels = jnp.searchsorted(jnp.cumsum(sizes), jnp.arange(rows * top), side="right").astype(jnp.int32)
    listing = labels.reshape(top, rows).T
    listing = listing[jax.random.permutation(jax.random.fold_in(own, 1), rows)]
    offset_by = jax.random.randint(jax.random.fold_in(own, 2), (rows, 1), 0, top)
    return jnp.take_along_axis(listing, (jnp.arange(top)[None, :] + offset_by) % top, axis=1)


def load_shares(number_of, total, limit, skew, full):
    loads = [(1 << 20) // math.isqrt(rank ** skew) + 1 for rank in range(1, number_of + 1)]
    largest = limit if full else min(limit, max(-(-total // number_of), total * loads[0] // sum(loads)))
    least = 1 if total - largest >= number_of - 1 else 0
    given, surplus = [largest] + [least] * (number_of - 1), total - largest - least * (number_of - 1)
    while surplus > 0:
        movable = [i for i in range(1, number_of) if given[i] < largest] or [i for i in range(1, number_of) if given[i] < limit]
        mass, left = sum([loads[i] for i in movable]), surplus
        for i in movable:
            extra = min(limit - given[i], max(1, left * loads[i] // mass), surplus)
            given[i] = given[i] + extra
            surplus = surplus - extra
    return np.array(given)


def centred(stream_key, shape, width, limit, split=(), held_as=jnp.bfloat16):
    gain = level_of(stream_key, shape, split, -0.22, 0.18) if split else 1.0
    entries = jax.random.normal(stream_key, shape, jnp.float32) * width * gain
    return jnp.minimum(jnp.maximum(entries, -limit), limit).astype(held_as)


def setup_inputs(seed: int = 0, part: int = 0) -> dict:
    streams_of = jax.random.split(jax.random.key(seed), 8)
    own_keys = jax.random.split(jax.random.fold_in(streams_of[7], part), 8)
    tokens = centred(own_keys[0], (TOKENS, D), 1.0, 6.0, ((0, 16),))
    norm_gain = jnp.clip(1.0 + 0.18 * jax.random.normal(streams_of[1], (D,), jnp.float32), 0.1, 1.9)
    router_weight = centred(streams_of[2], (D, EXPERTS), D ** -0.5, 0.1875)
    expert_ids_keys = jax.random.split(jax.random.fold_in(own_keys[3], 1), TOKENS // TOK_DEV)
    expert_ids_turns = jax.random.permutation(jax.random.fold_in(own_keys[3], 3), TOKENS // TOK_DEV)
    expert_ids = jax.vmap(lambda own, number: shared_out(jax.random.fold_in(own_keys[3], 2), own, number, TOK_DEV, EXPERTS, TOP, CAP, 2))(expert_ids_keys, expert_ids_turns).reshape((TOKENS, TOP))
    w_gate = centred(streams_of[4], (EXPERTS, D, FF), D ** -0.5, 0.1875, ((0, 16),))
    w_up = centred(streams_of[5], (EXPERTS, D, FF), D ** -0.5, 0.1875, ((0, 16),))
    w_down = centred(streams_of[6], (EXPERTS, FF, D), FF ** -0.5, 0.25, ((0, 16),))
    return {"tokens": tokens, "norm_gain": norm_gain, "router_weight": router_weight, "expert_ids": expert_ids, "w_gate": w_gate, "w_up": w_up, "w_down": w_down}


epsilon = 1e-05

def normalize(tokens, norm_gain):
    values = tokens.astype(jnp.float32)
    inverse = lax.rsqrt(lax.optimization_barrier(jnp.mean(values * values, axis=1, keepdims=True)) + epsilon)
    return (values * inverse * norm_gain).astype(jnp.bfloat16)

def gate_values(normed, router_weight, expert_ids):
    logits = jnp.dot(normed, router_weight, preferred_element_type=jnp.float32)
    chosen = jnp.take_along_axis(logits, expert_ids, axis=1)
    return jax.nn.softmax(chosen, axis=1)

def reference(tokens, norm_gain, router_weight, expert_ids, w_gate, w_up, w_down):
    normed = normalize(tokens, norm_gain)
    gates = gate_values(normed, router_weight, expert_ids)
    choices_total = TOKENS * TOP
    flat_ids = expert_ids.reshape(choices_total).astype(jnp.int32)
    flat_gates = gates.reshape(choices_total)
    positions = jnp.arange(choices_total, dtype=jnp.int32)
    most_rows = N_EP * CAP

    def one_expert(running, inputs):
        gate_matrix, up_matrix, down_matrix, expert_number = inputs
        keyed = jnp.where(flat_ids == expert_number, positions, jnp.int32(choices_total))
        picked = jnp.sort(keyed)[:most_rows]
        valid = picked < choices_total
        clipped = jnp.minimum(picked, choices_total - 1).astype(jnp.int32)
        rows = (clipped // TOP).astype(jnp.int32)
        weight = jnp.where(valid, flat_gates[clipped], jnp.float32(0.0))
        chosen_rows = normed[rows]
        gate_part = jnp.dot(chosen_rows, gate_matrix, preferred_element_type=jnp.float32)
        up_part = jnp.dot(chosen_rows, up_matrix, preferred_element_type=jnp.float32)
        hidden = (jax.nn.silu(gate_part) * up_part).astype(jnp.bfloat16)
        produced = jnp.dot(hidden, down_matrix, preferred_element_type=jnp.float32)
        return (running.at[rows].add(weight[:, None] * produced), None)
    no_sums = jnp.zeros((normed.shape[0], normed.shape[1]), jnp.float32)
    numbers = jnp.arange(EXPERTS, dtype=jnp.int32)
    running, _ = lax.scan(one_expert, no_sums, (w_gate, w_up, w_down, numbers))
    return running.astype(jnp.bfloat16)
```

```python
import jax
import jax.numpy as jnp
from jax import lax
from jax.sharding import PartitionSpec as P

epsilon = 1e-05


def normalize(tokens, norm_gain):
    values = tokens.astype(jnp.float32)
    inverse = lax.rsqrt(jnp.mean(values * values, axis=1, keepdims=True) + epsilon)
    return (values * inverse * norm_gain).astype(jnp.bfloat16)


def combine_of(normed, router_weight, expert_ids, expert):
    logits = jnp.dot(normed, router_weight, preferred_element_type=jnp.float32)
    numbers = lax.broadcasted_iota(jnp.int32, logits.shape, 1)
    hits = [numbers == expert_ids[:, k:k + 1] for k in range(expert_ids.shape[1])]
    chosen = jnp.stack([jnp.sum(jnp.where(h, logits, 0.0), axis=1) for h in hits], axis=1)
    gates = jax.nn.softmax(chosen, axis=1)
    return jnp.sum(jnp.where(expert_ids == expert, gates, 0.0), axis=1, keepdims=True)


def expert_output(block_rows, gate_matrix, up_matrix, down_matrix):
    gate_part = jnp.dot(block_rows, gate_matrix, preferred_element_type=jnp.float32)
    up_part = jnp.dot(block_rows, up_matrix, preferred_element_type=jnp.float32)
    hidden = (jax.nn.silu(gate_part) * up_part).astype(jnp.bfloat16)
    return jnp.dot(hidden, down_matrix, preferred_element_type=jnp.float32)


def shards(tokens, norm_gain, router_weight, expert_ids, w_gate, w_up, w_down):
    local_count = w_gate.shape[0]
    me = lax.axis_index("ep")
    normed = normalize(tokens, norm_gain)
    all_rows = lax.all_gather(normed, "ep", axis=0, tiled=True)
    all_ids = lax.all_gather(expert_ids, "ep", axis=0, tiled=True)
    total = None
    for within in range(local_count):
        weight = combine_of(all_rows, router_weight, all_ids, me * local_count + within)
        produced = expert_output(all_rows, w_gate[within], w_up[within], w_down[within])
        term = jnp.where(weight > 0, weight * produced, 0.0)
        total = term if total is None else total + term
    finished = lax.psum_scatter(total, "ep", scatter_dimension=0, tiled=True)
    return finished.astype(jnp.bfloat16)


def solution(mesh):
    return jax.shard_map(
        shards,
        mesh=mesh,
        in_specs=(
            P(("dp", "ep"), None),
            P(),
            P(),
            P(("dp", "ep"), None),
            P("ep", None, None),
            P("ep", None, None),
            P("ep", None, None),
        ),
        out_specs=P(("dp", "ep"), None),
        check_vma=False,
    )
```

```python
import functools

import jax
import jax.numpy as jnp
from jax import lax
from jax.experimental import pallas as pl
from jax.experimental.pallas import tpu as pltpu
from jax.sharding import PartitionSpec as P

epsilon = 1e-05
LANES = 128
SIDE = 2


def pack_rows(tokens_ref, gain_ref, router_ref, ids_ref):
    values = tokens_ref[...].astype(jnp.float32)
    inverse = lax.rsqrt(jnp.mean(values * values, axis=1, keepdims=True) + epsilon)
    normed = (values * inverse * gain_ref[...]).astype(jnp.bfloat16)
    logits = jnp.dot(normed, router_ref[...], preferred_element_type=jnp.float32)
    top = ids_ref.shape[1]
    numbers = lax.broadcasted_iota(jnp.int32, logits.shape, 1)
    ids = [ids_ref[:, k:k + 1] for k in range(top)]
    chosen = [jnp.sum(jnp.where(numbers == one, logits, 0.0), axis=1, keepdims=True) for one in ids]
    peak = functools.reduce(jnp.maximum, chosen)
    powers = [jnp.exp(one - peak) for one in chosen]
    total = sum(powers[1:], powers[0])
    lane = lax.broadcasted_iota(jnp.int32, (normed.shape[0], LANES), 1)
    extra = jnp.zeros((normed.shape[0], LANES), jnp.float32)
    for k in range(top):
        extra = jnp.where(lane == k, ids[k].astype(jnp.float32), extra)
        rest = powers[k] / total
        for piece in range(3):
            rounded = rest.astype(jnp.bfloat16).astype(jnp.float32)
            extra = jnp.where(lane == (piece + 1) * top + k, rounded, extra)
            rest = rest - rounded
    return normed, extra.astype(jnp.bfloat16)


def kernel(count, top, tokens_ref, gain_ref, router_ref, ids_ref, gate_hbm, up_hbm, down_hbm, out_ref,
           rows, part, from_core, from_x, from_z, w_gate, w_up, w_down,
           w_sem, ag_z_send, ag_z_recv, ag_x_send, ag_x_recv, ag_c_send, ag_c_recv,
           rs_c_send, rs_c_recv, rs_x_send, rs_x_recv, rs_z_send, rs_z_recv):
    planes = count // (SIDE * SIDE)
    me = lax.axis_index("ep")
    z, x, c = me // (SIDE * SIDE), (me // SIDE) % SIDE, me % SIDE
    local = w_gate.shape[0]
    width = out_ref.shape[1]

    def device(pz, px, pc):
        return {"ep": (pz * SIDE + px) * SIDE + pc}

    def remote(src, dst, send, recv, target):
        return pltpu.make_async_remote_copy(src_ref=src, dst_ref=dst, send_sem=send, recv_sem=recv,
                                            device_id=target, device_id_type=pl.DeviceIdType.MESH)

    x_mate, c_mate = device(z, 1 - x, c), device(z, x, 1 - c)
    z_up = [device((z + k) % planes, x, c) for k in range(planes)]
    source = [(z + planes - k) % planes for k in range(planes)]

    weights = [pltpu.make_async_copy(a, b, w_sem.at[i]) for i, (a, b) in
               enumerate([(gate_hbm, w_gate), (up_hbm, w_up), (down_hbm, w_down)])]
    for one in weights:
        one.start()
    barrier = pltpu.get_barrier_semaphore()
    for target in [x_mate, c_mate] + z_up[1:]:
        pl.semaphore_signal(barrier, inc=1, device_id=target, device_id_type=pl.DeviceIdType.MESH)
    normed, extra = pack_rows(tokens_ref, gain_ref, router_ref, ids_ref)
    rows[z, c, x, :, :width] = normed
    rows[z, c, x, :, width:] = extra
    pl.semaphore_wait(barrier, planes + 1)

    sends = []

    def go(copy):
        copy.start()
        sends.append(copy)
        return copy

    def block(k, px, pc):
        return rows.at[source[k], pc, px]

    ag_z = [None] + [go(remote(rows.at[z, c, x], rows.at[z, c, x], ag_z_send.at[k], ag_z_recv.at[k], z_up[k]))
                     for k in range(1, planes)]

    def ag_x(k):
        return remote(block(k, x, c), block(k, x, c), ag_x_send.at[k], ag_x_recv.at[k], x_mate)

    def ag_c(k, j):
        px = x if j == 0 else 1 - x
        return remote(block(k, px, c), block(k, px, c), ag_c_send.at[k, j], ag_c_recv.at[k, j], c_mate)

    def stage_a(k):
        if k:
            remote(block(k, x, c), block(k, x, c), ag_z_send.at[k], ag_z_recv.at[k], z_up[k]).wait_recv()
        go(ag_x(k))
        go(ag_c(k, 0))

    def stage_b(k):
        remote(block(k, 1 - x, c), block(k, 1 - x, c), ag_x_send.at[k], ag_x_recv.at[k], x_mate).wait_recv()
        go(ag_c(k, 1))

    def rs_c(k):
        return remote(part.at[k, 1 - c], from_core.at[k], rs_c_send.at[k], rs_c_recv.at[k], c_mate)

    def rs_x(k):
        return remote(part.at[k, c, 1 - x], from_x.at[k], rs_x_send.at[k], rs_x_recv.at[k], x_mate)

    def rs_z(k):
        return remote(part.at[k, c, x], from_z.at[k], rs_z_send.at[k], rs_z_recv.at[k], device(source[k], x, c))

    def stage_c(k):
        for j in range(SIDE):
            px = x if j == 0 else 1 - x
            remote(block(k, px, 1 - c), block(k, px, 1 - c), ag_c_send.at[k, j], ag_c_recv.at[k, j],
                   c_mate).wait_recv()
        if k == 0:
            for one in weights:
                one.wait()
        held = rows[source[k]].reshape(-1, width + LANES)
        data, extra = held[:, :width], held[:, width:].astype(jnp.float32)
        total = None
        for within in range(local):
            expert = (me * local + within).astype(jnp.float32)
            gate_part = jnp.dot(data, w_gate[within], preferred_element_type=jnp.float32)
            up_part = jnp.dot(data, w_up[within], preferred_element_type=jnp.float32)
            hidden = (gate_part / (1.0 + jnp.exp(-gate_part)) * up_part).astype(jnp.bfloat16)
            produced = jnp.dot(hidden, w_down[within], preferred_element_type=jnp.float32)
            weight = jnp.zeros((held.shape[0], 1), jnp.float32)
            for i in range(top):
                gate = sum(extra[:, (p + 1) * top + i:(p + 1) * top + i + 1] for p in range(3))
                weight = weight + jnp.where(extra[:, i:i + 1] == expert, gate, 0.0)
            term = produced * weight
            total = term if total is None else total + term
        part[k] = total.reshape(part.shape[1:])
        go(rs_c(k))

    def stage_d(k):
        rs_c(k).wait_recv()
        part[k, c, 1 - x] = part[k, c, 1 - x] + from_core[k, 1 - x]
        go(rs_x(k))
        part[k, c, x] = part[k, c, x] + from_core[k, x]

    def stage_e(k):
        rs_x(k).wait_recv()
        part[k, c, x] = part[k, c, x] + from_x[k]
        if k:
            go(rs_z(k))

    stages = {"a": stage_a, "b": stage_b, "c": stage_c, "d": stage_d, "e": stage_e}
    lag = {"b": 0, "a": 1, "c": 0, "d": 0, "e": -2}
    stage_a(0)
    for t in range(planes + 2):
        for name, shift in lag.items():
            if 0 <= t + shift < planes and (name != "a" or t + shift):
                stages[name](t + shift)
    total = part[0, c, x]
    for k in range(1, planes):
        rs_z(k).wait_recv()
        total = total + from_z[k]
    out_ref[...] = total.astype(out_ref.dtype)
    for copy in sends:
        copy.wait_send()


def solution(mesh):
    count = mesh.shape["ep"]

    def shards(tokens, norm_gain, router_weight, expert_ids, w_gate, w_up, w_down):
        size, width = tokens.shape
        planes = count // (SIDE * SIDE)
        top = expert_ids.shape[1]
        dma = pltpu.SemaphoreType.DMA
        vmem = pl.BlockSpec(memory_space=pltpu.VMEM)
        anywhere = pl.BlockSpec(memory_space=pl.ANY)
        f32 = jnp.float32
        return pl.pallas_call(
            functools.partial(kernel, count, top),
            out_shape=jax.ShapeDtypeStruct((size, width), jnp.bfloat16),
            in_specs=[vmem] * 4 + [anywhere] * 3,
            out_specs=vmem,
            scratch_shapes=[
                pltpu.VMEM((planes, SIDE, SIDE, size, width + LANES), jnp.bfloat16),
                pltpu.VMEM((planes, SIDE, SIDE, size, width), f32),
                pltpu.VMEM((planes, SIDE, size, width), f32),
                pltpu.VMEM((planes, size, width), f32),
                pltpu.VMEM((planes, size, width), f32),
                pltpu.VMEM(w_gate.shape, w_gate.dtype),
                pltpu.VMEM(w_up.shape, w_up.dtype),
                pltpu.VMEM(w_down.shape, w_down.dtype),
                dma((3,)), dma((planes,)), dma((planes,)), dma((planes,)), dma((planes,)),
                dma((planes, SIDE)), dma((planes, SIDE)),
                dma((planes,)), dma((planes,)), dma((planes,)), dma((planes,)), dma((planes,)), dma((planes,)),
            ],
            compiler_params=pltpu.CompilerParams(collective_id=0, has_side_effects=True,
                                                 vmem_limit_bytes=60 * 1024 * 1024),
        )(tokens, norm_gain.reshape(1, width), router_weight, expert_ids, w_gate, w_up, w_down)

    return jax.shard_map(
        shards,
        mesh=mesh,
        in_specs=(
            P(("dp", "ep"), None),
            P(),
            P(),
            P(("dp", "ep"), None),
            P("ep", None, None),
            P("ep", None, None),
            P("ep", None, None),
        ),
        out_specs=P(("dp", "ep"), None),
        check_vma=False,
    )
```

```python
import functools

import jax
import jax.numpy as jnp
from jax import lax
from jax.experimental import pallas as pl
from jax.experimental.pallas import tpu as pltpu
from jax.sharding import PartitionSpec as P

epsilon = 1e-05
LANES = 128
SIDE = 2


def pack_rows(tokens_ref, gain_ref, router_ref, ids_ref):
    values = tokens_ref[...].astype(jnp.float32)
    inverse = lax.rsqrt(jnp.mean(values * values, axis=1, keepdims=True) + epsilon)
    normed = (values * inverse * gain_ref[...]).astype(jnp.bfloat16)
    logits = jnp.dot(normed, router_ref[...], preferred_element_type=jnp.float32)
    top = ids_ref.shape[1]
    numbers = lax.broadcasted_iota(jnp.int32, logits.shape, 1)
    ids = [ids_ref[:, k:k + 1] for k in range(top)]
    chosen = [jnp.sum(jnp.where(numbers == one, logits, 0.0), axis=1, keepdims=True) for one in ids]
    peak = functools.reduce(jnp.maximum, chosen)
    powers = [jnp.exp(one - peak) for one in chosen]
    total = sum(powers[1:], powers[0])
    lane = lax.broadcasted_iota(jnp.int32, (normed.shape[0], LANES), 1)
    extra = jnp.zeros((normed.shape[0], LANES), jnp.float32)
    for k in range(top):
        extra = jnp.where(lane == k, ids[k].astype(jnp.float32), extra)
        rest = powers[k] / total
        for piece in range(3):
            rounded = rest.astype(jnp.bfloat16).astype(jnp.float32)
            extra = jnp.where(lane == (piece + 1) * top + k, rounded, extra)
            rest = rest - rounded
    return normed, extra.astype(jnp.bfloat16)


def kernel(count, top, tokens_ref, gain_ref, router_ref, ids_ref, gate_hbm, up_hbm, down_hbm, out_ref,
           rows, part, from_core, from_x, from_z, w_gate, w_up, w_down,
           w_sem, ag_z_send, ag_z_recv, ag_x_send, ag_x_recv, ag_c_send, ag_c_recv,
           rs_c_send, rs_c_recv, rs_x_send, rs_x_recv, rs_z_send, rs_z_recv):
    planes = count // (SIDE * SIDE)
    me = lax.axis_index("ep")
    z, x, c = me // (SIDE * SIDE), (me // SIDE) % SIDE, me % SIDE
    local = w_gate.shape[0]
    width = out_ref.shape[1]

    def device(pz, px, pc):
        return {"ep": (pz * SIDE + px) * SIDE + pc}

    def remote(src, dst, send, recv, target):
        return pltpu.make_async_remote_copy(src_ref=src, dst_ref=dst, send_sem=send, recv_sem=recv,
                                            device_id=target, device_id_type=pl.DeviceIdType.MESH)

    x_mate, c_mate = device(z, 1 - x, c), device(z, x, 1 - c)
    z_up = [device((z + k) % planes, x, c) for k in range(planes)]
    source = [(z + planes - k) % planes for k in range(planes)]

    weights = [pltpu.make_async_copy(a, b, w_sem.at[i]) for i, (a, b) in
               enumerate([(gate_hbm, w_gate), (up_hbm, w_up), (down_hbm, w_down)])]
    for one in weights:
        one.start()
    barrier = pltpu.get_barrier_semaphore()
    for target in [x_mate, c_mate] + z_up[1:]:
        pl.semaphore_signal(barrier, inc=1, device_id=target, device_id_type=pl.DeviceIdType.MESH)
    normed, extra = pack_rows(tokens_ref, gain_ref, router_ref, ids_ref)
    rows[z, c, x, :, :width] = normed
    rows[z, c, x, :, width:] = extra
    pl.semaphore_wait(barrier, planes + 1)

    sends = []

    def go(copy):
        copy.start()
        sends.append(copy)
        return copy

    def block(k, px, pc):
        return rows.at[source[k], pc, px]

    ag_z = [None] + [go(remote(rows.at[z, c, x], rows.at[z, c, x], ag_z_send.at[k], ag_z_recv.at[k], z_up[k]))
                     for k in range(1, planes)]

    def ag_x(k):
        return remote(block(k, x, c), block(k, x, c), ag_x_send.at[k], ag_x_recv.at[k], x_mate)

    def ag_c(k, j):
        px = x if j == 0 else 1 - x
        return remote(block(k, px, c), block(k, px, c), ag_c_send.at[k, j], ag_c_recv.at[k, j], c_mate)

    def stage_a(k):
        if k:
            remote(block(k, x, c), block(k, x, c), ag_z_send.at[k], ag_z_recv.at[k], z_up[k]).wait_recv()
        go(ag_x(k))
        go(ag_c(k, 0))

    def stage_b(k):
        remote(block(k, 1 - x, c), block(k, 1 - x, c), ag_x_send.at[k], ag_x_recv.at[k], x_mate).wait_recv()
        go(ag_c(k, 1))

    def rs_c(k):
        return remote(part.at[k, 1 - c], from_core.at[k], rs_c_send.at[k], rs_c_recv.at[k], c_mate)

    def rs_x(k):
        return remote(part.at[k, c, 1 - x], from_x.at[k], rs_x_send.at[k], rs_x_recv.at[k], x_mate)

    def rs_z(k):
        return remote(part.at[k, c, x], from_z.at[k], rs_z_send.at[k], rs_z_recv.at[k], device(source[k], x, c))

    def stage_c(k):
        for j in range(SIDE):
            px = x if j == 0 else 1 - x
            remote(block(k, px, 1 - c), block(k, px, 1 - c), ag_c_send.at[k, j], ag_c_recv.at[k, j],
                   c_mate).wait_recv()
        if k == 0:
            for one in weights:
                one.wait()
        held = rows[source[k]].reshape(-1, width + LANES)
        data, extra = held[:, :width], held[:, width:].astype(jnp.float32)
        total = None
        for within in range(local):
            expert = (me * local + within).astype(jnp.float32)
            gate_part = jnp.dot(data, w_gate[within], preferred_element_type=jnp.float32)
            up_part = jnp.dot(data, w_up[within], preferred_element_type=jnp.float32)
            hidden = (gate_part / (1.0 + jnp.exp(-gate_part)) * up_part).astype(jnp.bfloat16)
            produced = jnp.dot(hidden, w_down[within], preferred_element_type=jnp.float32)
            weight = jnp.zeros((held.shape[0], 1), jnp.float32)
            for i in range(top):
                gate = sum(extra[:, (p + 1) * top + i:(p + 1) * top + i + 1] for p in range(3))
                weight = weight + jnp.where(extra[:, i:i + 1] == expert, gate, 0.0)
            term = produced * weight
            total = term if total is None else total + term
        part[k] = total.reshape(part.shape[1:])
        go(rs_c(k))

    def stage_d(k):
        rs_c(k).wait_recv()
        part[k, c, 1 - x] = part[k, c, 1 - x] + from_core[k, 1 - x]
        go(rs_x(k))
        part[k, c, x] = part[k, c, x] + from_core[k, x]

    def stage_e(k):
        rs_x(k).wait_recv()
        part[k, c, x] = part[k, c, x] + from_x[k]
        if k:
            go(rs_z(k))

    stage_a(0)
    stage_b(0)
    stage_c(0)
    if planes > 1:
        stage_a(1)
    for k in range(1, planes):
        if k + 1 < planes:
            stage_a(k + 1)
        stage_b(k)
        stage_c(k)
        stage_d(k)
        if k > 1:
            stage_e(k - 1)
    stage_d(0)
    if planes > 1:
        stage_e(planes - 1)
    stage_e(0)
    total = part[0, c, x]
    for k in range(1, planes):
        rs_z(k).wait_recv()
        total = total + from_z[k]
    out_ref[...] = total.astype(out_ref.dtype)
    for copy in sends:
        copy.wait_send()


def solution(mesh):
    count = mesh.shape["ep"]

    def shards(tokens, norm_gain, router_weight, expert_ids, w_gate, w_up, w_down):
        size, width = tokens.shape
        planes = count // (SIDE * SIDE)
        top = expert_ids.shape[1]
        dma = pltpu.SemaphoreType.DMA
        vmem = pl.BlockSpec(memory_space=pltpu.VMEM)
        anywhere = pl.BlockSpec(memory_space=pl.ANY)
        f32 = jnp.float32
        return pl.pallas_call(
            functools.partial(kernel, count, top),
            out_shape=jax.ShapeDtypeStruct((size, width), jnp.bfloat16),
            in_specs=[vmem] * 4 + [anywhere] * 3,
            out_specs=vmem,
            scratch_shapes=[
                pltpu.VMEM((planes, SIDE, SIDE, size, width + LANES), jnp.bfloat16),
                pltpu.VMEM((planes, SIDE, SIDE, size, width), f32),
                pltpu.VMEM((planes, SIDE, size, width), f32),
                pltpu.VMEM((planes, size, width), f32),
                pltpu.VMEM((planes, size, width), f32),
                pltpu.VMEM(w_gate.shape, w_gate.dtype),
                pltpu.VMEM(w_up.shape, w_up.dtype),
                pltpu.VMEM(w_down.shape, w_down.dtype),
                dma((3,)), dma((planes,)), dma((planes,)), dma((planes,)), dma((planes,)),
                dma((planes, SIDE)), dma((planes, SIDE)),
                dma((planes,)), dma((planes,)), dma((planes,)), dma((planes,)), dma((planes,)), dma((planes,)),
            ],
            compiler_params=pltpu.CompilerParams(collective_id=0, has_side_effects=True,
                                                 vmem_limit_bytes=60 * 1024 * 1024),
        )(tokens, norm_gain.reshape(1, width), router_weight, expert_ids, w_gate, w_up, w_down)

    return jax.shard_map(
        shards,
        mesh=mesh,
        in_specs=(
            P(("dp", "ep"), None),
            P(),
            P(),
            P(("dp", "ep"), None),
            P("ep", None, None),
            P("ep", None, None),
            P("ep", None, None),
        ),
        out_specs=P(("dp", "ep"), None),
        check_vma=False,
    )
```

```python
import functools

import jax
import jax.numpy as jnp
from jax import lax
from jax.experimental import pallas as pl
from jax.experimental.pallas import tpu as pltpu
from jax.sharding import PartitionSpec as P

epsilon = 1e-05
LANES = 128
SIDE = 2
STEPS = 32000.0


def pack_rows(tokens_ref, gain_ref, router_ref, ids_ref):
    values = tokens_ref[...].astype(jnp.float32)
    inverse = lax.rsqrt(jnp.mean(values * values, axis=1, keepdims=True) + epsilon)
    normed = (values * inverse * gain_ref[...]).astype(jnp.bfloat16)
    logits = jnp.dot(normed, router_ref[...], preferred_element_type=jnp.float32)
    top = ids_ref.shape[1]
    numbers = lax.broadcasted_iota(jnp.int32, logits.shape, 1)
    ids = [ids_ref[:, k:k + 1] for k in range(top)]
    chosen = [jnp.sum(jnp.where(numbers == one, logits, 0.0), axis=1, keepdims=True) for one in ids]
    peak = functools.reduce(jnp.maximum, chosen)
    powers = [jnp.exp(one - peak) for one in chosen]
    total = sum(powers[1:], powers[0])
    lane = lax.broadcasted_iota(jnp.int32, (normed.shape[0], LANES), 1)
    extra = jnp.zeros((normed.shape[0], LANES), jnp.float32)
    for k in range(top):
        extra = jnp.where(lane == k, ids[k].astype(jnp.float32), extra)
        rest = powers[k] / total
        for piece in range(3):
            rounded = rest.astype(jnp.bfloat16).astype(jnp.float32)
            extra = jnp.where(lane == (piece + 1) * top + k, rounded, extra)
            rest = rest - rounded
    return normed, extra.astype(jnp.bfloat16)


def scale_of(exponent):
    return jnp.exp(exponent * 0.6931471805599453)


def encode(ref, values):
    width = values.shape[1]
    peak = jnp.maximum(jnp.max(jnp.abs(values), axis=1, keepdims=True), 1e-30)
    exponent = jnp.ceil(jnp.log(peak) * 1.4426950408889634)
    ref[:, :width] = jnp.round(values * (STEPS / scale_of(exponent))).astype(jnp.int32).astype(jnp.int16)
    ref[:, width:] = jnp.broadcast_to(exponent, (values.shape[0], LANES)).astype(jnp.int32).astype(jnp.int16)


def decode(ref, width):
    exponent = ref[:, width:].astype(jnp.int32).astype(jnp.float32)[:, :1]
    return ref[:, :width].astype(jnp.int32).astype(jnp.float32) * (scale_of(exponent) * (1.0 / STEPS))


def kernel(count, top, tokens_ref, gain_ref, router_ref, ids_ref, gate_hbm, up_hbm, down_hbm, out_ref,
           rows, part, from_core, to_x, from_x, to_z, from_z, w_gate, w_up, w_down,
           w_sem, ag_z_send, ag_z_recv, ag_x_send, ag_x_recv, ag_c_send, ag_c_recv,
           rs_c_send, rs_c_recv, rs_x_send, rs_x_recv, rs_z_send, rs_z_recv):
    planes = count // (SIDE * SIDE)
    me = lax.axis_index("ep")
    z, x, c = me // (SIDE * SIDE), (me // SIDE) % SIDE, me % SIDE
    local = w_gate.shape[0]
    width = out_ref.shape[1]

    def device(pz, px, pc):
        return {"ep": (pz * SIDE + px) * SIDE + pc}

    def remote(src, dst, send, recv, target):
        return pltpu.make_async_remote_copy(src_ref=src, dst_ref=dst, send_sem=send, recv_sem=recv,
                                            device_id=target, device_id_type=pl.DeviceIdType.MESH)

    x_mate, c_mate = device(z, 1 - x, c), device(z, x, 1 - c)
    z_up = [device((z + k) % planes, x, c) for k in range(planes)]
    source = [(z + planes - k) % planes for k in range(planes)]

    weights = [pltpu.make_async_copy(a, b, w_sem.at[i]) for i, (a, b) in
               enumerate([(gate_hbm, w_gate), (up_hbm, w_up), (down_hbm, w_down)])]
    for one in weights:
        one.start()
    barrier = pltpu.get_barrier_semaphore()
    for target in [x_mate, c_mate] + z_up[1:]:
        pl.semaphore_signal(barrier, inc=1, device_id=target, device_id_type=pl.DeviceIdType.MESH)
    normed, extra = pack_rows(tokens_ref, gain_ref, router_ref, ids_ref)
    rows[z, c, x, :, :width] = normed
    rows[z, c, x, :, width:] = extra
    pl.semaphore_wait(barrier, planes + 1)

    sends = []

    def go(copy):
        copy.start()
        sends.append(copy)
        return copy

    def block(k, px, pc):
        return rows.at[source[k], pc, px]

    ag_z = [None] + [go(remote(rows.at[z, c, x], rows.at[z, c, x], ag_z_send.at[k], ag_z_recv.at[k], z_up[k]))
                     for k in range(1, planes)]

    def ag_x(k):
        return remote(block(k, x, c), block(k, x, c), ag_x_send.at[k], ag_x_recv.at[k], x_mate)

    def ag_c(k, j):
        px = x if j == 0 else 1 - x
        return remote(block(k, px, c), block(k, px, c), ag_c_send.at[k, j], ag_c_recv.at[k, j], c_mate)

    def stage_a(k):
        if k:
            remote(block(k, x, c), block(k, x, c), ag_z_send.at[k], ag_z_recv.at[k], z_up[k]).wait_recv()
        go(ag_x(k))
        go(ag_c(k, 0))

    def stage_b(k):
        remote(block(k, 1 - x, c), block(k, 1 - x, c), ag_x_send.at[k], ag_x_recv.at[k], x_mate).wait_recv()
        go(ag_c(k, 1))

    def rs_c(k):
        return remote(part.at[k, 1 - c], from_core.at[k], rs_c_send.at[k], rs_c_recv.at[k], c_mate)

    def rs_x(k):
        return remote(to_x.at[k], from_x.at[k], rs_x_send.at[k], rs_x_recv.at[k], x_mate)

    def rs_z(k):
        return remote(to_z.at[k], from_z.at[k], rs_z_send.at[k], rs_z_recv.at[k], device(source[k], x, c))

    def stage_c(k):
        for j in range(SIDE):
            px = x if j == 0 else 1 - x
            remote(block(k, px, 1 - c), block(k, px, 1 - c), ag_c_send.at[k, j], ag_c_recv.at[k, j],
                   c_mate).wait_recv()
        if k == 0:
            for one in weights:
                one.wait()
        held = rows[source[k]].reshape(-1, width + LANES)
        data, extra = held[:, :width], held[:, width:].astype(jnp.float32)
        total = None
        for within in range(local):
            expert = (me * local + within).astype(jnp.float32)
            gate_part = jnp.dot(data, w_gate[within], preferred_element_type=jnp.float32)
            up_part = jnp.dot(data, w_up[within], preferred_element_type=jnp.float32)
            hidden = (gate_part / (1.0 + jnp.exp(-gate_part)) * up_part).astype(jnp.bfloat16)
            produced = jnp.dot(hidden, w_down[within], preferred_element_type=jnp.float32)
            weight = jnp.zeros((held.shape[0], 1), jnp.float32)
            for i in range(top):
                gate = sum(extra[:, (p + 1) * top + i:(p + 1) * top + i + 1] for p in range(3))
                weight = weight + jnp.where(extra[:, i:i + 1] == expert, gate, 0.0)
            term = produced * weight
            total = term if total is None else total + term
        part[k] = total.reshape(part.shape[1:])
        go(rs_c(k))

    def stage_d(k):
        rs_c(k).wait_recv()
        encode(to_x.at[k], part[k, c, 1 - x] + from_core[k, 1 - x])
        go(rs_x(k))

    def stage_e(k):
        rs_x(k).wait_recv()
        whole = part[k, c, x] + from_core[k, x] + decode(from_x.at[k], width)
        if k == 0:
            return whole
        encode(to_z.at[k], whole)
        go(rs_z(k))

    stage_a(0)
    stage_b(0)
    stage_c(0)
    if planes > 1:
        stage_a(1)
    for k in range(1, planes):
        if k + 1 < planes:
            stage_a(k + 1)
        stage_b(k)
        stage_c(k)
        stage_d(k)
        if k > 1:
            stage_e(k - 1)
    stage_d(0)
    if planes > 1:
        stage_e(planes - 1)
    total = stage_e(0)
    for k in range(1, planes):
        rs_z(k).wait_recv()
        total = total + decode(from_z.at[k], width)
    out_ref[...] = total.astype(out_ref.dtype)
    for copy in sends:
        copy.wait_send()


def solution(mesh):
    count = mesh.shape["ep"]

    def shards(tokens, norm_gain, router_weight, expert_ids, w_gate, w_up, w_down):
        size, width = tokens.shape
        planes = count // (SIDE * SIDE)
        top = expert_ids.shape[1]
        dma = pltpu.SemaphoreType.DMA
        vmem = pl.BlockSpec(memory_space=pltpu.VMEM)
        anywhere = pl.BlockSpec(memory_space=pl.ANY)
        f32 = jnp.float32
        return pl.pallas_call(
            functools.partial(kernel, count, top),
            out_shape=jax.ShapeDtypeStruct((size, width), jnp.bfloat16),
            in_specs=[vmem] * 4 + [anywhere] * 3,
            out_specs=vmem,
            scratch_shapes=[
                pltpu.VMEM((planes, SIDE, SIDE, size, width + LANES), jnp.bfloat16),
                pltpu.VMEM((planes, SIDE, SIDE, size, width), f32),
                pltpu.VMEM((planes, SIDE, size, width), f32),
                pltpu.VMEM((planes, size, width + LANES), jnp.int16),
                pltpu.VMEM((planes, size, width + LANES), jnp.int16),
                pltpu.VMEM((planes, size, width + LANES), jnp.int16),
                pltpu.VMEM((planes, size, width + LANES), jnp.int16),
                pltpu.VMEM(w_gate.shape, w_gate.dtype),
                pltpu.VMEM(w_up.shape, w_up.dtype),
                pltpu.VMEM(w_down.shape, w_down.dtype),
                dma((3,)), dma((planes,)), dma((planes,)), dma((planes,)), dma((planes,)),
                dma((planes, SIDE)), dma((planes, SIDE)),
                dma((planes,)), dma((planes,)), dma((planes,)), dma((planes,)), dma((planes,)), dma((planes,)),
            ],
            compiler_params=pltpu.CompilerParams(collective_id=0, has_side_effects=True,
                                                 vmem_limit_bytes=60 * 1024 * 1024),
        )(tokens, norm_gain.reshape(1, width), router_weight, expert_ids, w_gate, w_up, w_down)

    return jax.shard_map(
        shards,
        mesh=mesh,
        in_specs=(
            P(("dp", "ep"), None),
            P(),
            P(),
            P(("dp", "ep"), None),
            P("ep", None, None),
            P("ep", None, None),
            P("ep", None, None),
        ),
        out_specs=P(("dp", "ep"), None),
        check_vma=False,
    )
```

```python
import functools

import jax
import jax.numpy as jnp
from jax import lax
from jax.experimental import pallas as pl
from jax.experimental.pallas import tpu as pltpu
from jax.sharding import PartitionSpec as P

epsilon = 1e-05
LANES = 128
SIDE = 2
STEPS = 32000.0


def pack_rows(tokens_ref, gain_ref, router_ref, ids_ref):
    values = tokens_ref[...].astype(jnp.float32)
    inverse = lax.rsqrt(jnp.mean(values * values, axis=1, keepdims=True) + epsilon)
    normed = (values * inverse * gain_ref[...]).astype(jnp.bfloat16)
    logits = lax.dot_general(normed, router_ref[...], (((1,), (1,)), ((), ())), preferred_element_type=jnp.float32)
    top, size = ids_ref.shape
    diagonal = (lax.broadcasted_iota(jnp.int32, (size, size), 0) == lax.broadcasted_iota(jnp.int32, (size, size), 1))
    numbers = lax.broadcasted_iota(jnp.int32, logits.shape, 1).astype(jnp.float32)
    ids = [jnp.sum(jnp.where(diagonal, ids_ref[k:k + 1, :], 0).astype(jnp.float32), axis=1, keepdims=True)
           for k in range(top)]
    chosen = [jnp.sum(jnp.where(numbers == one, logits, 0.0), axis=1, keepdims=True) for one in ids]
    peak = functools.reduce(jnp.maximum, chosen)
    powers = [jnp.exp(one - peak) for one in chosen]
    total = sum(powers[1:], powers[0])
    lane = lax.broadcasted_iota(jnp.int32, (normed.shape[0], LANES), 1)
    extra = jnp.zeros((normed.shape[0], LANES), jnp.float32)
    for k in range(top):
        extra = jnp.where(lane == k, ids[k], extra)
        rest = powers[k] / total
        for piece in range(3):
            rounded = rest.astype(jnp.bfloat16).astype(jnp.float32)
            extra = jnp.where(lane == (piece + 1) * top + k, rounded, extra)
            rest = rest - rounded
    return normed, extra.astype(jnp.bfloat16)


def scale_of(exponent):
    return jnp.exp(exponent * 0.6931471805599453)


def encode(ref, values):
    width = values.shape[1]
    peak = jnp.maximum(jnp.max(jnp.abs(values), axis=1, keepdims=True), 1e-30)
    exponent = jnp.ceil(jnp.log(peak) * 1.4426950408889634)
    ref[:, :width] = jnp.round(values * (STEPS / scale_of(exponent))).astype(jnp.int32).astype(jnp.int16)
    ref[:, width:] = jnp.broadcast_to(exponent, (values.shape[0], LANES)).astype(jnp.int32).astype(jnp.int16)


def decode(ref, width):
    exponent = ref[:, width:].astype(jnp.int32).astype(jnp.float32)[:, :1]
    return ref[:, :width].astype(jnp.int32).astype(jnp.float32) * (scale_of(exponent) * (1.0 / STEPS))


def kernel(count, top, tokens_ref, gain_ref, router_ref, ids_ref, gate_hbm, up_hbm, down_hbm, out_ref,
           rows, part, from_core, to_x, from_x, to_z, from_z, w_gate, w_up, w_down,
           w_sem, ag_z_send, ag_z_recv, ag_x_send, ag_x_recv, ag_c_send, ag_c_recv,
           rs_c_send, rs_c_recv, rs_x_send, rs_x_recv, rs_z_send, rs_z_recv):
    planes = count // (SIDE * SIDE)
    me = lax.axis_index("ep")
    z, x, c = me // (SIDE * SIDE), (me // SIDE) % SIDE, me % SIDE
    local = w_gate.shape[0]
    width = out_ref.shape[1]

    def device(pz, px, pc):
        return {"ep": (pz * SIDE + px) * SIDE + pc}

    def remote(src, dst, send, recv, target):
        return pltpu.make_async_remote_copy(src_ref=src, dst_ref=dst, send_sem=send, recv_sem=recv,
                                            device_id=target, device_id_type=pl.DeviceIdType.MESH)

    x_mate, c_mate = device(z, 1 - x, c), device(z, x, 1 - c)
    z_up = [device((z + k) % planes, x, c) for k in range(planes)]
    source = [(z + planes - k) % planes for k in range(planes)]

    weights = [pltpu.make_async_copy(a, b, w_sem.at[i]) for i, (a, b) in
               enumerate([(gate_hbm, w_gate), (up_hbm, w_up), (down_hbm, w_down)])]
    for one in weights:
        one.start()
    barrier = pltpu.get_barrier_semaphore()
    for target in [x_mate, c_mate] + z_up[1:]:
        pl.semaphore_signal(barrier, inc=1, device_id=target, device_id_type=pl.DeviceIdType.MESH)
    normed, extra = pack_rows(tokens_ref, gain_ref, router_ref, ids_ref)
    rows[z, c, x, :, :width] = normed
    rows[z, c, x, :, width:] = extra
    pl.semaphore_wait(barrier, planes + 1)

    sends = []

    def go(copy):
        copy.start()
        sends.append(copy)
        return copy

    def block(k, px, pc):
        return rows.at[source[k], pc, px]

    ag_z = [None] + [go(remote(rows.at[z, c, x], rows.at[z, c, x], ag_z_send.at[k], ag_z_recv.at[k], z_up[k]))
                     for k in range(1, planes)]

    def ag_x(k):
        return remote(block(k, x, c), block(k, x, c), ag_x_send.at[k], ag_x_recv.at[k], x_mate)

    def ag_c(k, j):
        px = x if j == 0 else 1 - x
        return remote(block(k, px, c), block(k, px, c), ag_c_send.at[k, j], ag_c_recv.at[k, j], c_mate)

    def stage_a(k):
        if k:
            remote(block(k, x, c), block(k, x, c), ag_z_send.at[k], ag_z_recv.at[k], z_up[k]).wait_recv()
        go(ag_x(k))
        go(ag_c(k, 0))

    def stage_b(k):
        remote(block(k, 1 - x, c), block(k, 1 - x, c), ag_x_send.at[k], ag_x_recv.at[k], x_mate).wait_recv()
        go(ag_c(k, 1))

    def rs_c(k):
        return remote(part.at[k, 1 - c], from_core.at[k], rs_c_send.at[k], rs_c_recv.at[k], c_mate)

    def rs_x(k):
        return remote(to_x.at[k], from_x.at[k], rs_x_send.at[k], rs_x_recv.at[k], x_mate)

    def rs_z(k):
        return remote(to_z.at[k], from_z.at[k], rs_z_send.at[k], rs_z_recv.at[k], device(source[k], x, c))

    def stage_c(k):
        for j in range(SIDE):
            px = x if j == 0 else 1 - x
            remote(block(k, px, 1 - c), block(k, px, 1 - c), ag_c_send.at[k, j], ag_c_recv.at[k, j],
                   c_mate).wait_recv()
        if k == 0:
            for one in weights:
                one.wait()
        held = rows[source[k]].reshape(-1, width + LANES)
        data, extra = held[:, :width], held[:, width:].astype(jnp.float32)
        total = None
        for within in range(local):
            expert = (me * local + within).astype(jnp.float32)
            gate_part = jnp.dot(data, w_gate[within], preferred_element_type=jnp.float32)
            up_part = jnp.dot(data, w_up[within], preferred_element_type=jnp.float32)
            hidden = (gate_part / (1.0 + jnp.exp(-gate_part)) * up_part).astype(jnp.bfloat16)
            produced = jnp.dot(hidden, w_down[within], preferred_element_type=jnp.float32)
            weight = jnp.zeros((held.shape[0], 1), jnp.float32)
            for i in range(top):
                gate = sum(extra[:, (p + 1) * top + i:(p + 1) * top + i + 1] for p in range(3))
                weight = weight + jnp.where(extra[:, i:i + 1] == expert, gate, 0.0)
            term = produced * weight
            total = term if total is None else total + term
        part[k] = total.reshape(part.shape[1:])
        go(rs_c(k))

    def stage_d(k):
        rs_c(k).wait_recv()
        encode(to_x.at[k], part[k, c, 1 - x] + from_core[k, 1 - x])
        go(rs_x(k))

    def stage_e(k):
        rs_x(k).wait_recv()
        whole = part[k, c, x] + from_core[k, x] + decode(from_x.at[k], width)
        if k == 0:
            return whole
        encode(to_z.at[k], whole)
        go(rs_z(k))

    stage_a(0)
    stage_b(0)
    stage_c(0)
    for k in range(1, min(3, planes)):
        stage_a(k)
    if planes > 1:
        stage_b(1)
    for k in range(1, planes):
        stage_c(k)
        if k + 2 < planes:
            stage_a(k + 2)
        if k > 1:
            stage_e(k - 1)
        stage_d(k)
        if k + 1 < planes:
            stage_b(k + 1)
    stage_d(0)
    if planes > 1:
        stage_e(planes - 1)
    total = stage_e(0)
    for k in range(1, planes):
        rs_z(k).wait_recv()
        total = total + decode(from_z.at[k], width)
    out_ref[...] = total.astype(out_ref.dtype)
    for copy in sends:
        copy.wait_send()


def solution(mesh):
    count = mesh.shape["ep"]

    def shards(tokens, norm_gain, router_weight, expert_ids, w_gate, w_up, w_down):
        size, width = tokens.shape
        planes = count // (SIDE * SIDE)
        top = expert_ids.shape[1]
        dma = pltpu.SemaphoreType.DMA
        vmem = pl.BlockSpec(memory_space=pltpu.VMEM)
        anywhere = pl.BlockSpec(memory_space=pl.ANY)
        f32 = jnp.float32
        return pl.pallas_call(
            functools.partial(kernel, count, top),
            out_shape=jax.ShapeDtypeStruct((size, width), jnp.bfloat16),
            in_specs=[vmem] * 4 + [anywhere] * 3,
            out_specs=vmem,
            scratch_shapes=[
                pltpu.VMEM((planes, SIDE, SIDE, size, width + LANES), jnp.bfloat16),
                pltpu.VMEM((planes, SIDE, SIDE, size, width), f32),
                pltpu.VMEM((planes, SIDE, size, width), f32),
                pltpu.VMEM((planes, size, width + LANES), jnp.int16),
                pltpu.VMEM((planes, size, width + LANES), jnp.int16),
                pltpu.VMEM((planes, size, width + LANES), jnp.int16),
                pltpu.VMEM((planes, size, width + LANES), jnp.int16),
                pltpu.VMEM(w_gate.shape, w_gate.dtype),
                pltpu.VMEM(w_up.shape, w_up.dtype),
                pltpu.VMEM(w_down.shape, w_down.dtype),
                dma((3,)), dma((planes,)), dma((planes,)), dma((planes,)), dma((planes,)),
                dma((planes, SIDE)), dma((planes, SIDE)),
                dma((planes,)), dma((planes,)), dma((planes,)), dma((planes,)), dma((planes,)), dma((planes,)),
            ],
            compiler_params=pltpu.CompilerParams(collective_id=0, has_side_effects=True,
                                                 vmem_limit_bytes=60 * 1024 * 1024),
        )(tokens, norm_gain.reshape(1, width), router_weight.T, expert_ids.T, w_gate, w_up, w_down)

    return jax.shard_map(
        shards,
        mesh=mesh,
        in_specs=(
            P(("dp", "ep"), None),
            P(),
            P(),
            P(("dp", "ep"), None),
            P("ep", None, None),
            P("ep", None, None),
            P("ep", None, None),
        ),
        out_specs=P(("dp", "ep"), None),
        check_vma=False,
    )
```
